8 devices in a mesh: data: 4 (over z, y, x), expert: 2 (over core).
Axes of the slice: x: 2, y: 2, z: 1, core: 2. Of those that a mesh axis runs over, the one named last changes fastest.
Arguments:
- dy: bfloat16 [32768, 768], P(('data', 'expert'))
- gates: float32 [32768, 1], P(('data', 'expert'))
- topk_idx: int32 [32768, 1], P(('data', 'expert'))
- slot: int32 [32768, 1], P(('data', 'expert'))
- yd: bfloat16 [32768, 1, 768], P(('data', 'expert'))
- xd: bfloat16 [32, 1280, 768], P(('data', 'expert'))
- h1: bfloat16 [32, 1280, 3072], P(('data', 'expert'))
- h3: bfloat16 [32, 1280, 3072], P(('data', 'expert'))
- w1: bfloat16 [8, 768, 3072], P('expert')
- w3: bfloat16 [8, 768, 3072], P('expert')
- w2: bfloat16 [8, 3072, 768], P('expert')
Outputs:
- output 1: bfloat16 [32768, 768], P(('data', 'expert'))
- output 2: float32 [32768, 1], P(('data', 'expert'))
- output 3: float32 [8, 768, 3072], P('expert', None, 'data')
- output 4: float32 [8, 768, 3072], P('expert', None, 'data')
- output 5: float32 [8, 3072, 768], P('expert', 'data')
All inputs are finite; a program needn't handle non-finite values.
Results may differ from the reference program's by a relative error of at most 0.0106909.
Values are sent between devices in bfloat16 or wider.
A program may use at most 1 GiB of HBM per device.

```python
import jax
import jax.numpy as jnp
from jax import lax

NDATA = 4
NEXP = 2
TOKENS = 4096
EXPERTS = 8
TOPK = 1
DMODEL = 768
FF = 3072
CAP = 640

NTOK = NDATA * NEXP * TOKENS
NDEV = NDATA * NEXP
NBUF = NEXP * CAP


def _routes(topk_idx, slot):
    dev = jnp.arange(NTOK, dtype=jnp.int32) // TOKENS
    row = (dev // NEXP)[:, None] * EXPERTS + topk_idx
    col = jnp.where(slot >= 0, (dev % NEXP)[:, None] * CAP + slot, NBUF)
    return row, col


def _slots(topk_idx):
    def one(idx):
        oh = (idx.reshape(-1)[:, None] == jnp.arange(EXPERTS, dtype=jnp.int32)[None, :]).astype(jnp.int32)
        rank = jnp.sum((jnp.cumsum(oh, axis=0) - oh) * oh, axis=1)
        return jnp.where(rank < CAP, rank, -1).reshape(TOKENS, TOPK)
    return lax.map(one, topk_idx.reshape(NDEV, TOKENS, TOPK)).reshape(NTOK, TOPK).astype(jnp.int32)


def _forward(x, topk_idx, slot, w1, w3, w2):
    row, col = _routes(topk_idx, slot)
    xin = jnp.broadcast_to(x[:, None, :], (NTOK, TOPK, DMODEL))
    xd = jnp.zeros((NDATA * EXPERTS, NBUF, DMODEL), jnp.bfloat16).at[row, col].set(xin, mode='drop')
    x4 = xd.reshape(NDATA, EXPERTS, NBUF, DMODEL)

    def one(e):
        xs = x4[:, e].reshape(NDATA * NBUF, DMODEL)
        h1 = jnp.dot(xs, w1[e], preferred_element_type=jnp.float32).astype(jnp.bfloat16)
        h3 = jnp.dot(xs, w3[e], preferred_element_type=jnp.float32).astype(jnp.bfloat16)
        h1f = h1.astype(jnp.float32)
        a = (h1f * jax.nn.sigmoid(h1f) * h3.astype(jnp.float32)).astype(jnp.bfloat16)
        y = jnp.dot(a, w2[e], preferred_element_type=jnp.float32).astype(jnp.bfloat16)
        return h1.reshape(NDATA, NBUF, FF), h3.reshape(NDATA, NBUF, FF), y.reshape(NDATA, NBUF, DMODEL)

    h1, h3, y = lax.map(one, jnp.arange(EXPERTS))
    flat = lambda a: jnp.swapaxes(a, 0, 1).reshape(NDATA * EXPERTS, NBUF, a.shape[-1])
    h1, h3, y = flat(h1), flat(h3), flat(y)
    yd = jnp.where((slot >= 0)[:, :, None], y[row, jnp.minimum(col, NBUF - 1)], jnp.zeros((), jnp.bfloat16))
    return xd, h1, h3, yd


def _draw_routes(bias_key, pick_key):
    level_parts = jax.random.randint(bias_key, (4, NDEV, EXPERTS), 0, 4, jnp.int32)
    levels = jnp.sum(level_parts, axis=0)
    weights = jnp.left_shift(jnp.ones_like(levels), levels)
    tok_dev = jnp.arange(NTOK, dtype=jnp.int32) // TOKENS
    row_weights = weights[tok_dev]
    pick_keys = jax.random.split(pick_key, TOPK)
    columns = jnp.arange(EXPERTS, dtype=jnp.int32)[None, :]
    chosen = []
    for choice_idx in range(TOPK):
        bounds = jnp.cumsum(row_weights, axis=1)
        draw_value = jax.random.randint(pick_keys[choice_idx], (NTOK,), 0, bounds[:, -1], jnp.int32)
        pick_now = jnp.sum(bounds <= draw_value[:, None], axis=1, dtype=jnp.int32)
        chosen.append(pick_now)
        row_weights = jnp.where(columns == pick_now[:, None], 0, row_weights)
    return jnp.stack(chosen, axis=1).astype(jnp.int32)


def setup_inputs(seed: int = 0) -> dict:
    ks = jax.random.split(jax.random.PRNGKey(seed), 8)
    x = jax.random.normal(ks[0], (NTOK, DMODEL), jnp.float32).astype(jnp.bfloat16)
    w1 = (jax.random.normal(ks[1], (EXPERTS, DMODEL, FF), jnp.float32) * DMODEL ** -0.5).astype(jnp.bfloat16)
    w3 = (jax.random.normal(ks[2], (EXPERTS, DMODEL, FF), jnp.float32) * DMODEL ** -0.5).astype(jnp.bfloat16)
    w2 = (jax.random.normal(ks[3], (EXPERTS, FF, DMODEL), jnp.float32) * FF ** -0.5).astype(jnp.bfloat16)
    rk = jax.random.split(jax.random.fold_in(ks[4], 7), 2)
    topk_idx = _draw_routes(rk[0], rk[1])
    slot = _slots(topk_idx)
    gates = jax.random.uniform(ks[5], (NTOK, TOPK), jnp.float32, 0.2, 1.0)
    dy = jax.random.normal(ks[6], (NTOK, DMODEL), jnp.float32).astype(jnp.bfloat16)
    xd, h1, h3, yd = _forward(x, topk_idx, slot, w1, w3, w2)
    return dict(dy=dy, gates=gates, topk_idx=topk_idx, slot=slot, yd=yd, xd=xd, h1=h1, h3=h3, w1=w1, w3=w3, w2=w2)


def reference(dy, gates, topk_idx, slot, yd, xd, h1, h3, w1, w3, w2):
    row, col = _routes(topk_idx, slot)
    dyf = dy.astype(jnp.float32)
    dg = jnp.sum(yd.astype(jnp.float32) * dyf[:, None, :], axis=-1)
    v = (gates[:, :, None] * dyf[:, None, :]).astype(jnp.bfloat16)
    dyd = jnp.zeros((NDATA * EXPERTS, NBUF, DMODEL), jnp.bfloat16).at[row, col].set(v, mode='drop')
    grp = lambda a: a.reshape(NDATA, EXPERTS, NBUF, a.shape[-1])
    g4, x4, a14, a34 = grp(dyd), grp(xd), grp(h1), grp(h3)

    def one(e):
        g = g4[:, e].reshape(NDATA * NBUF, DMODEL)
        x = x4[:, e].reshape(NDATA * NBUF, DMODEL)
        h1f = a14[:, e].reshape(NDATA * NBUF, FF).astype(jnp.float32)
        h3f = a34[:, e].reshape(NDATA * NBUF, FF).astype(jnp.float32)
        s = jax.nn.sigmoid(h1f)
        silu = h1f * s
        a = (silu * h3f).astype(jnp.bfloat16)
        da = jnp.dot(g, w2[e].T, preferred_element_type=jnp.float32).astype(jnp.bfloat16).astype(jnp.float32)
        dh1 = (da * h3f * s * (1.0 + h1f * (1.0 - s))).astype(jnp.bfloat16)
        dh3 = (da * silu).astype(jnp.bfloat16)
        dw2 = jnp.dot(a.T, g, preferred_element_type=jnp.float32)
        dw1 = jnp.dot(x.T, dh1, preferred_element_type=jnp.float32)
        dw3 = jnp.dot(x.T, dh3, preferred_element_type=jnp.float32)
        dxd = (jnp.dot(dh1, w1[e].T, preferred_element_type=jnp.float32)
               + jnp.dot(dh3, w3[e].T, preferred_element_type=jnp.float32)).astype(jnp.bfloat16)
        return dw1, dw3, dw2, dxd.reshape(NDATA, NBUF, DMODEL)

    dw1, dw3, dw2, dxd = lax.map(one, jnp.arange(EXPERTS))
    dxd = jnp.swapaxes(dxd, 0, 1).reshape(NDATA * EXPERTS, NBUF, DMODEL)
    back = dxd[row, jnp.minimum(col, NBUF - 1)].astype(jnp.float32)
    dx = jnp.sum(jnp.where((slot >= 0)[:, :, None], back, 0.0), axis=1).astype(jnp.bfloat16)
    return dx, dg, dw1, dw3, dw2
```

```python
import jax
import jax.numpy as jnp
from jax import lax
from jax.sharding import PartitionSpec as P

F32 = jnp.float32
BF16 = jnp.bfloat16


def _act(da, h1, h3):
    h1f = h1.astype(F32)
    h3f = h3.astype(F32)
    s = jax.nn.sigmoid(h1f)
    silu = h1f * s
    a = (silu * h3f).astype(BF16)
    dh1 = (da * h3f * s * (1.0 + h1f * (1.0 - s))).astype(BF16)
    dh3 = (da * silu).astype(BF16)
    return a, dh1, dh3


def _share(x, g, w1, w3, w2):
    h1 = jnp.einsum('ecd,edf->ecf', x, w1, preferred_element_type=F32).astype(BF16)
    h3 = jnp.einsum('ecd,edf->ecf', x, w3, preferred_element_type=F32).astype(BF16)
    da = jnp.einsum('ecd,efd->ecf', g, w2, preferred_element_type=F32).astype(BF16).astype(F32)
    a, dh1, dh3 = _act(da, h1, h3)
    return (jnp.einsum('ecd,ecf->edf', x, dh1, preferred_element_type=F32),
            jnp.einsum('ecd,ecf->edf', x, dh3, preferred_element_type=F32),
            jnp.einsum('ecf,ecd->efd', a, g, preferred_element_type=F32))


def solution(mesh):
    np_ = mesh.shape['expert']
    nd = mesh.shape['data']
    tok = P(('data', 'expert'), None)
    buf = P(('data', 'expert'), None, None)
    wsp = P('expert', None, None)

    def hop(v, bit):
        return lax.ppermute(v, 'data', [(i, i ^ bit) for i in range(nd)])

    def spread(v):
        half = v.shape[0] // 2
        lo, hi = v[:half], v[half:]
        xlo, xhi, ylo, yhi = hop(lo, 1), hop(hi, 1), hop(lo, 2), hop(hi, 2)
        return (lo, xlo, ylo, hop(ylo, 1)), (hi, xhi, yhi, hop(xhi, 2))

    def body(dy, gates, topk_idx, slot, yd, xd, h1, h3, w1, w3, w2):
        d = dy.shape[1]
        el = w1.shape[0]
        cap = xd.shape[1] // np_
        xs = spread(xd)
        v = (gates[:, :, None] * dy.astype(F32)[:, None, :]).astype(BF16)
        col = jnp.where(slot >= 0, slot, cap)
        send = jnp.zeros((np_ * el, cap, d), BF16).at[topk_idx, col].set(v, mode='drop')
        recv = lax.all_to_all(send.reshape(np_, el, cap, d), 'expert', 0, 0, tiled=True)
        dyd = jnp.swapaxes(recv, 0, 1).reshape(el, np_ * cap, d)
        gs = spread(dyd)
        dg = jnp.einsum('tkd,td->tk', yd, dy, preferred_element_type=F32)
        da = jnp.einsum('ecd,efd->ecf', dyd, w2, preferred_element_type=F32).astype(BF16).astype(F32)
        _, dh1, dh3 = _act(da, h1, h3)
        dxd = (jnp.einsum('ecf,edf->ecd', dh1, w1, preferred_element_type=F32)
               + jnp.einsum('ecf,edf->ecd', dh3, w3, preferred_element_type=F32)).astype(BF16)
        out = jnp.swapaxes(dxd.reshape(el, np_, cap, d), 0, 1)
        back = lax.all_to_all(out, 'expert', 0, 0, tiled=True).reshape(np_ * el, cap, d)
        got = back[topk_idx, jnp.minimum(col, cap - 1)].astype(F32)
        dx = jnp.sum(jnp.where((slot >= 0)[:, :, None], got, 0.0), axis=1).astype(BF16)

        fs = w1.shape[2] // nd
        f0 = lax.axis_index('data') * fs
        w1s = lax.dynamic_slice_in_dim(w1, f0, fs, 2)
        w3s = lax.dynamic_slice_in_dim(w3, f0, fs, 2)
        w2s = lax.dynamic_slice_in_dim(w2, f0, fs, 1)
        parts = []
        for h in range(2):
            ws = tuple(w[h * (el // 2):(h + 1) * (el // 2)] for w in (w1s, w3s, w2s))
            tot = None
            for x, g in zip(xs[h], gs[h]):
                p = _share(x, g, *ws)
                tot = p if tot is None else tuple(a + b for a, b in zip(tot, p))
            parts.append(tot)
        dw1, dw3, dw2 = (jnp.concatenate(p, axis=0) for p in zip(*parts))
        return dx, dg, dw1, dw3, dw2

    return jax.shard_map(body, mesh=mesh,
                         in_specs=(tok, tok, tok, tok, buf, buf, buf, buf, wsp, wsp, wsp),
                         out_specs=(tok, tok, P('expert', None, 'data'), P('expert', None, 'data'), P('expert', 'data', None)),
                         check_vma=False)
```

```python
import functools

import jax
import jax.numpy as jnp
from jax import lax
from jax.experimental import pallas as pl
from jax.experimental.pallas import tpu as pltpu
from jax.sharding import PartitionSpec as P

F32 = jnp.float32
BF16 = jnp.bfloat16
I32 = jnp.int32
RB = 256
AL = 32
VMEM_LIMIT = 62 * 1024 * 1024
ANY = pl.BlockSpec(memory_space=pl.ANY)


def _used(meta, ns, ne, el, g, j, r):
    e = meta[ns * ne]
    v = meta[(g * (ne // el) + jnp.bitwise_xor(e, r)) * ne + e * el + j]
    return jnp.bitwise_and(v + (AL - 1), -AL)


def _pack_kernel(dims, bounds, base_e, meta, src0, src1, *rest):
    ns, ne, el = dims
    nc = len(bounds) - 1
    outs, (lst, sem_in, sem_out) = rest[:nc], rest[nc:]
    total = bounds[-1]
    e = meta[ns * ne]
    d = meta[ns * ne + 1]

    def zero(i, c):
        lst[pl.ds(i * 64, 64), :] = jnp.zeros((64, lst.shape[1]), BF16)
        return c
    lax.fori_loop(0, total // 64, zero, 0)

    def walk(start):
        off = jnp.int32(0)
        for j in range(el):
            for r in range(2):
                src = (src0, src1)[r]
                n = _used(meta, ns, ne, el, d, j, r)
                cap = src0.shape[0] // el // (2 if base_e else 1)
                base = j * 2 * cap + jnp.bitwise_xor(e, r) * cap if base_e else jnp.int32(j * cap)
                nbig = n // 128
                for size, lo, cnt in ((128, 0, nbig), (AL, nbig * 128, (n - nbig * 128) // AL)):
                    def step(i, c, size=size, lo=lo, base=base, off=off, src=src):
                        p = lo + i * size
                        cp = pltpu.make_async_copy(src.at[pl.ds(pl.multiple_of(base + p, AL), size)],
                                                   lst.at[pl.ds(pl.multiple_of(off + p, AL), size)], sem_in)
                        if start:
                            cp.start()
                        else:
                            cp.wait()
                        return c
                    lax.fori_loop(0, cnt, step, 0)
                off = off + n
    walk(True)
    walk(False)
    cps = [pltpu.make_async_copy(lst.at[pl.ds(bounds[i], bounds[i + 1] - bounds[i])], outs[i], sem_out.at[i])
           for i in range(nc)]
    for cp in cps:
        cp.start()
    for cp in cps:
        cp.wait()


def _pack(meta, src0, src1, dims, bounds, base_e):
    w = src0.shape[1]
    nc = len(bounds) - 1
    return pl.pallas_call(
        functools.partial(_pack_kernel, dims, bounds, base_e),
        grid_spec=pltpu.PrefetchScalarGridSpec(
            num_scalar_prefetch=1, grid=(), in_specs=[ANY, ANY], out_specs=[ANY] * nc,
            scratch_shapes=[pltpu.VMEM((bounds[-1], w), BF16), pltpu.SemaphoreType.DMA, pltpu.SemaphoreType.DMA((nc,))]),
        out_shape=[jax.ShapeDtypeStruct((bounds[i + 1] - bounds[i], w), BF16) for i in range(nc)],
        compiler_params=pltpu.CompilerParams(vmem_limit_bytes=24 * 1024 * 1024),
        cost_estimate=pl.CostEstimate(flops=0, bytes_accessed=4 * bounds[-1] * w, transcendentals=0),
        name="pack",
    )(meta, src0, src1)


def _nt(a, b):
    return lax.dot_general(a, b, (((1,), (1,)), ((), ())), preferred_element_type=F32)


def _tn(a, b):
    return lax.dot_general(a, b, (((0,), (0,)), ((), ())), preferred_element_type=F32)


def _own_kernel(dims, cap, meta, g0, g1, h1, h3, w1, w3, w2, o0, o1, gb, h1b, h3b, acc, ob, items, sin, sout):
    ns, ne, el = dims
    j = pl.program_id(0)
    e = meta[ns * ne]
    d = meta[ns * ne + 1]
    ff = w1.shape[2]
    fc = w1.shape[1]

    cnt = jnp.int32(0)
    for r in range(2):
        n = _used(meta, ns, ne, el, d, j, r)
        nb = (n + RB - 1) // RB

        def put(b, c, r=r):
            items[c, 0] = r
            items[c, 1] = jnp.minimum(b * RB, cap - RB)
            return c + 1
        cnt = lax.fori_loop(0, nb, put, cnt)

    def copies(i, slot, op):
        r = items[i, 0]
        st = items[i, 1]
        row = pl.multiple_of(jnp.bitwise_xor(e, r) * cap + st, 128)
        for k, (src, dst) in enumerate(((h1, h1b), (h3, h3b))):
            op(pltpu.make_async_copy(src.at[j, pl.ds(row, RB)], dst.at[slot], sin.at[slot, k]))
        st = pl.multiple_of(st, 128)
        for q, g in enumerate((g0, g1)):
            @pl.when(r == q)
            def _():
                op(pltpu.make_async_copy(g.at[j, pl.ds(st, RB)], gb.at[slot], sin.at[slot, 2]))

    def out(i, slot, op):
        r = items[i, 0]
        st = pl.multiple_of(items[i, 1], 128)
        for q, o in enumerate((o0, o1)):
            @pl.when(r == q)
            def _():
                op(pltpu.make_async_copy(ob.at[slot], o.at[j, pl.ds(st, RB)], sout.at[slot]))

    start = lambda cp: cp.start()
    wait = lambda cp: cp.wait()

    @pl.when(cnt > 0)
    def _():
        copies(0, 0, start)

    def step(i, c):
        slot = lax.rem(i, 2)

        @pl.when(i + 1 < cnt)
        def _():
            copies(i + 1, 1 - slot, start)
        copies(i, slot, wait)
        @pl.when(i >= 1)
        def _():
            out(i - 1, 1 - slot, wait)
        g = gb[slot]

        def hid(k, c2):
            f = pl.multiple_of(k * fc, 128)
            da = _nt(g, w2[0, pl.ds(f, fc), :]).astype(BF16).astype(F32)
            h1f = h1b[slot, :, pl.ds(f, fc)].astype(F32)
            h3f = h3b[slot, :, pl.ds(f, fc)].astype(F32)
            s = jax.nn.sigmoid(h1f)
            dh1 = (da * h3f * s * (1.0 + h1f * (1.0 - s))).astype(BF16)
            dh3 = (da * (h1f * s)).astype(BF16)
            p = _nt(dh1, w1[0, :, pl.ds(f, fc)]) + _nt(dh3, w3[0, :, pl.ds(f, fc)])
            acc[...] = jnp.where(k == 0, p, acc[...] + p)
            return c2
        lax.fori_loop(0, ff // fc, hid, 0)
        ob[slot] = acc[...].astype(BF16)
        out(i, slot, start)
        return c
    lax.fori_loop(0, cnt, step, 0)

    @pl.when(cnt > 0)
    def _():
        out(cnt - 1, lax.rem(cnt - 1, 2), wait)


def _own(meta, g0, g1, h1, h3, w1, w3, w2, dims):
    el, cap, w = g0.shape
    ff = w1.shape[2]
    wspec = lambda a: pl.BlockSpec((1,) + a.shape[1:], lambda j, m: (j, 0, 0))
    return pl.pallas_call(
        functools.partial(_own_kernel, dims, cap),
        grid_spec=pltpu.PrefetchScalarGridSpec(
            num_scalar_prefetch=1, grid=(el,),
            in_specs=[ANY, ANY, ANY, ANY, wspec(w1), wspec(w3), wspec(w2)], out_specs=[ANY, ANY],
            scratch_shapes=[pltpu.VMEM((2, RB, w), BF16), pltpu.VMEM((2, RB, ff), BF16), pltpu.VMEM((2, RB, ff), BF16),
                            pltpu.VMEM((RB, w), F32), pltpu.VMEM((2, RB, w), BF16), pltpu.SMEM((16, 2), I32),
                            pltpu.SemaphoreType.DMA((2, 3)), pltpu.SemaphoreType.DMA((2,))]),
        out_shape=[jax.ShapeDtypeStruct(g0.shape, BF16)] * 2,
        compiler_params=pltpu.CompilerParams(vmem_limit_bytes=VMEM_LIMIT),
        cost_estimate=pl.CostEstimate(flops=4 * el * cap * w * ff * 3, bytes_accessed=el * (cap * ff * 4 + 3 * w * ff * 2), transcendentals=0),
        name="own",
    )(meta, g0, g1, h1, h3, w1, w3, w2)


def _share_kernel(dims, lo, first, meta, xs, gs, w1, w3, w2, *rest):
    ns, ne, el = dims
    if first:
        ins, rest = None, rest
    else:
        ins, rest = rest[:3], rest[3:]
    dw1, dw3, dw2, xb, gb, items, sin = rest
    j = pl.program_id(0)
    ng, c, w = xs.shape
    for k, o in enumerate((dw1, dw3, dw2)):
        o[...] = jnp.zeros_like(o) if first else ins[k][...]

    cnt = jnp.int32(0)
    for g in range(ng):
        pos = jnp.int32(0)
        for jj in range(el):
            n = _used(meta, ns, ne, el, g, jj, 0) + _used(meta, ns, ne, el, g, jj, 1)
            pos = pos + jnp.where(jj < j, n, 0)
        n = _used(meta, ns, ne, el, g, j, 0) + _used(meta, ns, ne, el, g, j, 1)
        a = jnp.clip(pos - lo, 0, c)
        z = jnp.clip(pos + n - lo, 0, c)

        def put(b, k, g=g, a=a, z=z):
            s = a + b * RB
            items[k, 0] = g
            items[k, 1] = jnp.minimum(s, c - RB)
            items[k, 2] = s
            items[k, 3] = jnp.minimum(s + RB, z)
            return k + 1
        cnt = lax.fori_loop(0, (z - a + RB - 1) // RB, put, cnt)

    def copies(i, slot, op):
        g = items[i, 0]
        st = pl.multiple_of(items[i, 1], AL)
        for k, (src, dst) in enumerate(((xs, xb), (gs, gb))):
            op(pltpu.make_async_copy(src.at[g, pl.ds(st, RB)], dst.at[slot], sin.at[slot, k]))

    start = lambda cp: cp.start()
    wait = lambda cp: cp.wait()

    @pl.when(cnt > 0)
    def _():
        copies(0, 0, start)

    def step(i, carry):
        slot = lax.rem(i, 2)

        @pl.when(i + 1 < cnt)
        def _():
            copies(i + 1, 1 - slot, start)
        copies(i, slot, wait)
        row = items[i, 1] + lax.broadcasted_iota(I32, (RB, w), 0)
        keep = (row >= items[i, 2]) & (row < items[i, 3])
        x = jnp.where(keep, xb[slot].astype(F32), 0.0).astype(BF16)
        g = jnp.where(keep, gb[slot].astype(F32), 0.0).astype(BF16)
        h1f = jnp.dot(x, w1[0], preferred_element_type=F32).astype(BF16).astype(F32)
        h3f = jnp.dot(x, w3[0], preferred_element_type=F32).astype(BF16).astype(F32)
        da = _nt(g, w2[0]).astype(BF16).astype(F32)
        s = jax.nn.sigmoid(h1f)
        silu = h1f * s
        a = (silu * h3f).astype(BF16)
        dh1 = (da * h3f * s * (1.0 + h1f * (1.0 - s))).astype(BF16)
        dh3 = (da * silu).astype(BF16)
        dw1[0] += _tn(x, dh1)
        dw3[0] += _tn(x, dh3)
        dw2[0] += _tn(a, g)
        return carry
    lax.fori_loop(0, cnt, step, 0)


def _share(meta, xs, gs, w1, w3, w2, prev, lo, dims):
    ns, ne, el = dims
    ng, c, w = xs.shape
    fs = w1.shape[2] // ng
    di = ns * ne + 1
    in_specs = [ANY, ANY,
                pl.BlockSpec((1, w, fs), lambda j, m: (j, 0, m[di])),
                pl.BlockSpec((1, w, fs), lambda j, m: (j, 0, m[di])),
                pl.BlockSpec((1, fs, w), lambda j, m: (j, m[di], 0))]
    acc = [pl.BlockSpec((1, w, fs), lambda j, m: (j, 0, 0)), pl.BlockSpec((1, w, fs), lambda j, m: (j, 0, 0)),
           pl.BlockSpec((1, fs, w), lambda j, m: (j, 0, 0))]
    first = prev is None
    args = (meta, xs, gs, w1, w3, w2) + (() if first else tuple(prev))
    return pl.pallas_call(
        functools.partial(_share_kernel, dims, lo, first),
        grid_spec=pltpu.PrefetchScalarGridSpec(
            num_scalar_prefetch=1, grid=(el,), in_specs=in_specs + ([] if first else acc), out_specs=acc,
            scratch_shapes=[pltpu.VMEM((2, RB, w), BF16), pltpu.VMEM((2, RB, w), BF16),
                            pltpu.SMEM((ng * (c // RB + 2), 4), I32), pltpu.SemaphoreType.DMA((2, 2))]),
        out_shape=[jax.ShapeDtypeStruct((el, w, fs), F32), jax.ShapeDtypeStruct((el, w, fs), F32),
                   jax.ShapeDtypeStruct((el, fs, w), F32)],
        input_output_aliases={} if first else {6: 0, 7: 1, 8: 2},
        compiler_params=pltpu.CompilerParams(vmem_limit_bytes=VMEM_LIMIT),
        cost_estimate=pl.CostEstimate(flops=8 * ng * c * w * fs, bytes_accessed=4 * ng * c * w, transcendentals=0),
        name="share",
    )(*args)


def _take_kernel(n0, tb, idx, d0, d1, o, buf, row):
    i = pl.program_id(0)
    n, w = d0.shape

    @pl.when(i == 0)
    def _():
        for k, s in enumerate((d0, d1)):
            def fill(b, c, k=k, s=s):
                buf[pl.ds(k * n + b * 64, 64), :] = s[pl.ds(b * 64, 64), :].astype(F32)
                return c
            lax.fori_loop(0, n // 64, fill, 0)
        buf[pl.ds(2 * n, 8), :] = jnp.zeros((8, w), F32)

    def step(t, c):
        for u in range(8):
            row[pl.ds(t * 8 + u, 1), :] = buf[pl.ds(idx[i * tb + t * 8 + u], 1), :]
        return c
    lax.fori_loop(0, tb // 8, step, 0)
    o[...] = row[...].astype(BF16)


def _take(idx, d0, d1, tb=512):
    n, w = d0.shape
    t = idx.shape[0]
    whole = pl.BlockSpec((n, w), lambda i, m: (0, 0), pipeline_mode=pl.Buffered(1))
    return pl.pallas_call(
        functools.partial(_take_kernel, n, tb),
        grid_spec=pltpu.PrefetchScalarGridSpec(
            num_scalar_prefetch=1, grid=(t // tb,), in_specs=[whole, whole],
            out_specs=pl.BlockSpec((tb, w), lambda i, m: (i, 0)),
            scratch_shapes=[pltpu.VMEM((2 * n + 8, w), F32), pltpu.VMEM((tb, w), F32)]),
        out_shape=jax.ShapeDtypeStruct((t, w), BF16),
        compiler_params=pltpu.CompilerParams(vmem_limit_bytes=48 * 1024 * 1024),
        cost_estimate=pl.CostEstimate(flops=20 * t * w, bytes_accessed=8 * n * w, transcendentals=0),
        name="take",
    )(idx, d0, d1)


def solution(mesh):
    np_ = mesh.shape['expert']
    nd = mesh.shape['data']
    tok = P(('data', 'expert'), None)
    buf = P(('data', 'expert'), None, None)
    wsp = P('expert', None, None)

    def body(dy, gates, topk_idx, slot, yd, xd, h1, h3, w1, w3, w2):
        t, d = dy.shape
        el = w1.shape[0]
        ne = np_ * el
        ns = nd * np_
        cap = xd.shape[1] // np_
        dims = (ns, ne, el)
        e = lax.axis_index('expert')
        dd = lax.axis_index('data')
        ex = topk_idx[:, 0]
        sl = slot[:, 0]
        hit = (ex[None, :] == jnp.arange(ne, dtype=I32)[:, None]) & (sl >= 0)[None, :]
        used = jnp.max(jnp.where(hit, sl[None, :] + 1, 0), axis=1).astype(I32)
        alld = lax.all_gather(used, ('data', 'expert'), axis=0, tiled=True)
        meta = jnp.concatenate([alld, e[None].astype(I32), dd[None].astype(I32)])
        rows = jnp.bitwise_and(alld + (AL - 1), -AL).reshape(nd, np_, np_, el).sum(axis=(1, 3))
        most = jnp.max(rows)
        rel = jnp.bitwise_xor(ex, e.astype(I32) * el)
        flat = jnp.where(sl >= 0, rel * cap + sl, ne * cap)

        def path(bounds, dy, gates, flat, yd, xd, h1, h3, w1, w3, w2, meta):
            x2 = xd.reshape(el * np_ * cap, d)
            xl = _pack(meta, x2, x2, dims, bounds, True)
            v = (gates * dy.astype(F32)).astype(BF16)
            send = jnp.zeros((ne * cap, d), BF16).at[flat].set(v, mode='drop').reshape(2, el, cap, d)
            g0 = send[0]
            g1 = lax.ppermute(send[1], 'expert', [(0, 1), (1, 0)])
            gl = _pack(meta, g0.reshape(el * cap, d), g1.reshape(el * cap, d), dims, bounds, False)
            xa, ga = [], []
            dep = None
            for k in range(len(bounds) - 1):
                xk = xl[k]
                if k > 0:
                    xk, _ = lax.optimization_barrier((xk, gl[k - 1]))
                xa.append(lax.all_gather(xk, 'data'))
                ga.append(lax.all_gather(gl[k], 'data'))
            o0, o1 = _own(meta, g0, g1, h1, h3, w1, w3, w2, dims)
            b1 = lax.ppermute(o1, 'expert', [(0, 1), (1, 0)])
            dx = _take(flat, o0.reshape(el * cap, d), b1.reshape(el * cap, d))
            dg = jnp.einsum('tkd,td->tk', yd, dy, preferred_element_type=F32)
            acc = None
            for k in range(len(bounds) - 1):
                acc = _share(meta, xa[k], ga[k], w1, w3, w2, acc, bounds[k], dims)
            return dx, dg, acc[0], acc[1], acc[2]

        small = (0, 1280, 2304, 3328)
        large = (0, 2560, 5120)
        ops = (dy, gates, flat, yd, xd, h1, h3, w1, w3, w2, meta)
        return lax.cond(most <= small[-1], functools.partial(path, small), functools.partial(path, large), *ops)

    return jax.shard_map(body, mesh=mesh,
                         in_specs=(tok, tok, tok, tok, buf, buf, buf, buf, wsp, wsp, wsp),
                         out_specs=(tok, tok, P('expert', None, 'data'), P('expert', None, 'data'), P('expert', 'data', None)),
                         check_vma=False)
```

```python
import functools

import jax
import jax.numpy as jnp
from jax import lax
from jax.experimental import pallas as pl
from jax.experimental.pallas import tpu as pltpu
from jax.sharding import PartitionSpec as P


F32 = jnp.float32
BF16 = jnp.bfloat16
I32 = jnp.int32
RB = 256
AL = 16
VMEM_LIMIT = 62 * 1024 * 1024
ANY = pl.BlockSpec(memory_space=pl.ANY)


def _used(meta, dims, g, j, r, other=0):
    ns, ne, el = dims
    e = jnp.bitwise_xor(meta[ns * ne], other)
    v = meta[(g * (ne // el) + jnp.bitwise_xor(e, r)) * ne + e * el + j]
    return jnp.bitwise_and(v + (AL - 1), -AL)


def _total(meta, dims, g):
    n = jnp.int32(0)
    for j in range(dims[2]):
        n = n + _used(meta, dims, g, j, 0) + _used(meta, dims, g, j, 1)
    return n


def _pack_kernel(dims, bounds, win, base_e, meta, src0, src1, *rest):
    ns, ne, el = dims
    nc = len(bounds) - 1 + (1 if win else 0)
    outs, (lst, sem_in, sem_out) = rest[:nc], rest[nc:]
    e = meta[ns * ne]
    d = meta[ns * ne + 1]

    def zero(i, c):
        lst[pl.ds(i * 64, 64), :] = jnp.zeros((64, lst.shape[1]), BF16)
        return c

    lax.fori_loop(0, lst.shape[0] // 64, zero, 0)

    def walk(start):
        off = jnp.int32(0)
        for j in range(el):
            for r in range(2):
                src = (src0, src1)[r]
                n = _used(meta, dims, d, j, r)
                cap = src0.shape[0] // el // (2 if base_e else 1)
                base = j * 2 * cap + jnp.bitwise_xor(e, r) * cap if base_e else jnp.int32(j * cap)
                nbig = n // 128
                for size, lo, cnt in ((128, 0, nbig), (AL, nbig * 128, (n - nbig * 128) // AL)):
                    def step(i, c, size=size, lo=lo, base=base, off=off, src=src):
                        p = lo + i * size
                        cp = pltpu.make_async_copy(src.at[pl.ds(pl.multiple_of(base + p, AL), size)],
                                                   lst.at[pl.ds(pl.multiple_of(off + p, AL), size)], sem_in)
                        if start:
                            cp.start()
                        else:
                            cp.wait()
                        return c

                    lax.fori_loop(0, cnt, step, 0)
                off = off + n
        return off

    walk(True)
    total = walk(False)
    cps = [pltpu.make_async_copy(lst.at[pl.ds(bounds[i], bounds[i + 1] - bounds[i])], outs[i], sem_out.at[i])
           for i in range(len(bounds) - 1)]
    if win:
        st = pl.multiple_of(jnp.clip(total - win, 0, lst.shape[0] - win), AL)
        cps.append(pltpu.make_async_copy(lst.at[pl.ds(st, win)], outs[nc - 1], sem_out.at[nc - 1]))
    for cp in cps:
        cp.start()
    for cp in cps:
        cp.wait()


def _pack(meta, src0, src1, dims, bounds, win, base_e):
    w = src0.shape[1]
    sizes = [b - a for a, b in zip(bounds, bounds[1:])] + ([win] if win else [])
    nc = len(sizes)
    rows = bounds[-1] + win
    return pl.pallas_call(
        functools.partial(_pack_kernel, dims, bounds, win, base_e),
        grid_spec=pltpu.PrefetchScalarGridSpec(
            num_scalar_prefetch=1, grid=(), in_specs=[ANY, ANY], out_specs=[ANY] * nc,
            scratch_shapes=[pltpu.VMEM((rows, w), BF16), pltpu.SemaphoreType.DMA, pltpu.SemaphoreType.DMA((nc,))]),
        out_shape=[jax.ShapeDtypeStruct((n, w), BF16) for n in sizes],
        compiler_params=pltpu.CompilerParams(vmem_limit_bytes=24 * 1024 * 1024),
        cost_estimate=pl.CostEstimate(flops=0, bytes_accessed=4 * rows * w, transcendentals=0),
        name="pack",
    )(meta, src0, src1)


def _extent_kernel(mesh_shape, ne, ex, sl, o, mine, sem_local, ssem, rsem):
    nd, npar = mesh_shape
    d = lax.axis_index('data')
    e = lax.axis_index('expert')
    lane = lax.broadcasted_iota(I32, (8, 128), 1)
    vec = jnp.zeros((8, 128), I32)
    idx = ex[...]
    pos = sl[...]
    for k in range(ne):
        top = jnp.max(jnp.where((idx == k) & (pos >= 0), pos + 1, 0))
        vec = jnp.where(lane == k, top, vec)
    mine[...] = vec
    bar = pltpu.get_barrier_semaphore()
    peers = [(a, b) for a in range(nd) for b in range(npar) if a or b]
    dev = lambda a, b: (jnp.bitwise_xor(d, a), jnp.bitwise_xor(e, b))
    for a, b in peers:
        pl.semaphore_signal(bar, inc=1, device_id=dev(a, b), device_id_type=pl.DeviceIdType.MESH)
    pl.semaphore_wait(bar, len(peers))
    me = d * npar + e
    cps = []
    for k, (a, b) in enumerate(peers):
        cp = pltpu.make_async_remote_copy(mine, o.at[me], ssem.at[k], rsem.at[k], device_id=dev(a, b),
                                          device_id_type=pl.DeviceIdType.MESH)
        cp.start()
        cps.append(cp)
    own = pltpu.make_async_copy(mine, o.at[me], sem_local)
    own.start()
    own.wait()
    for cp in cps:
        cp.wait()


def _extents(ex, sl, ne, mesh_shape):
    nd, npar = mesh_shape
    n = nd * npar
    rows = ex.shape[0] // 128
    vm = pl.BlockSpec(memory_space=pltpu.VMEM)
    out = pl.pallas_call(
        functools.partial(_extent_kernel, mesh_shape, ne),
        in_specs=[vm, vm], out_specs=vm,
        scratch_shapes=[pltpu.VMEM((8, 128), I32), pltpu.SemaphoreType.DMA, pltpu.SemaphoreType.DMA((n - 1,)),
                        pltpu.SemaphoreType.DMA((n - 1,))],
        out_shape=jax.ShapeDtypeStruct((n, 8, 128), I32),
        compiler_params=pltpu.CompilerParams(collective_id=0, has_side_effects=True),
        cost_estimate=pl.CostEstimate(flops=0, bytes_accessed=65536, transcendentals=0),
        name="extents",
    )(ex.reshape(rows, 128), sl.reshape(rows, 128))
    return out[:, 0, :ne].reshape(n * ne)


def _nt(a, b):
    return lax.dot_general(a, b, (((1,), (1,)), ((), ())), preferred_element_type=F32)


def _tn(a, b):
    return lax.dot_general(a, b, (((0,), (0,)), ((), ())), preferred_element_type=F32)


def _own_kernel(dims, cap, meta, g0, g1, h1, h3, w1, w3, w2, o0, o1, gb, h1b, h3b, ob, items, sin, sout):
    ns, ne, _ = dims
    j = pl.program_id(0)
    e = meta[ns * ne]
    d = meta[ns * ne + 1]
    ff = w1.shape[2]
    fc = w1.shape[1]

    cnt = jnp.int32(0)
    for r in range(2):
        n = _used(meta, dims, d, j, r)
        nb = (n + RB - 1) // RB

        def put(b, c, r=r):
            items[c, 0] = r
            items[c, 1] = jnp.minimum(b * RB, cap - RB)
            return c + 1

        cnt = lax.fori_loop(0, nb, put, cnt)

    def copies(i, slot, op):
        r = items[i, 0]
        st = items[i, 1]
        row = pl.multiple_of(jnp.bitwise_xor(e, r) * cap + st, 128)
        for k, (src, dst) in enumerate(((h1, h1b), (h3, h3b))):
            op(pltpu.make_async_copy(src.at[j, pl.ds(row, RB)], dst.at[slot], sin.at[slot, k]))
        st = pl.multiple_of(st, 128)
        for q, g in enumerate((g0, g1)):
            @pl.when(r == q)
            def _():
                op(pltpu.make_async_copy(g.at[j, pl.ds(st, RB)], gb.at[slot], sin.at[slot, 2]))

    def out(i, slot, op):
        r = items[i, 0]
        st = pl.multiple_of(items[i, 1], 128)
        for q, o in enumerate((o0, o1)):
            @pl.when(r == q)
            def _():
                op(pltpu.make_async_copy(ob.at[slot], o.at[j, pl.ds(st, RB)], sout.at[slot]))

    start = lambda cp: cp.start()
    wait = lambda cp: cp.wait()

    @pl.when(cnt > 0)
    def _():
        copies(0, 0, start)

    def step(i, c):
        slot = lax.rem(i, 2)

        @pl.when(i + 1 < cnt)
        def _():
            copies(i + 1, 1 - slot, start)

        copies(i, slot, wait)

        @pl.when(i >= 1)
        def _():
            out(i - 1, 1 - slot, wait)

        g = gb[slot]

        p = None
        for k in range(ff // fc):
            f = k * fc
            da = _nt(g, w2[0, f:f + fc, :]).astype(BF16).astype(F32)
            h1f = h1b[slot, :, f:f + fc].astype(F32)
            h3f = h3b[slot, :, f:f + fc].astype(F32)
            s = 0.5 * jnp.tanh(0.5 * h1f) + 0.5
            silu = h1f * s
            dh1 = (da * h3f * (s + silu * (1.0 - s))).astype(BF16)
            dh3 = (da * silu).astype(BF16)
            q = _nt(dh1, w1[0, :, f:f + fc]) + _nt(dh3, w3[0, :, f:f + fc])
            p = q if p is None else p + q
        ob[slot] = p.astype(BF16)
        out(i, slot, start)
        return c

    lax.fori_loop(0, cnt, step, 0)

    @pl.when(cnt > 0)
    def _():
        out(cnt - 1, lax.rem(cnt - 1, 2), wait)


def _own(meta, g0, g1, h1, h3, w1, w3, w2, dims):
    el, cap, w = g0.shape
    ff = w1.shape[2]
    wspec = lambda a: pl.BlockSpec((1,) + a.shape[1:], lambda j, m: (j, 0, 0))
    return pl.pallas_call(
        functools.partial(_own_kernel, dims, cap),
        grid_spec=pltpu.PrefetchScalarGridSpec(
            num_scalar_prefetch=1, grid=(el,),
            in_specs=[ANY, ANY, ANY, ANY, wspec(w1), wspec(w3), wspec(w2)], out_specs=[ANY, ANY],
            scratch_shapes=[pltpu.VMEM((2, RB, w), BF16), pltpu.VMEM((2, RB, ff), BF16), pltpu.VMEM((2, RB, ff), BF16),
                            pltpu.VMEM((2, RB, w), BF16), pltpu.SMEM((16, 2), I32),
                            pltpu.SemaphoreType.DMA((2, 3)), pltpu.SemaphoreType.DMA((2,))]),
        out_shape=[jax.ShapeDtypeStruct(g0.shape, BF16)] * 2,
        compiler_params=pltpu.CompilerParams(vmem_limit_bytes=VMEM_LIMIT),
        cost_estimate=pl.CostEstimate(flops=4 * el * cap * w * ff * 3, bytes_accessed=el * (cap * ff * 4 + 3 * w * ff * 2), transcendentals=0),
        name="own",
    )(meta, g0, g1, h1, h3, w1, w3, w2)


def _share_kernel(dims, parts, first, meta, *rest):
    ns, ne, el = dims
    na = len(parts)
    arrs, rest = rest[:2 * na], rest[2 * na:]
    (w1, w3, w2), rest = rest[:3], rest[3:]
    if first:
        ins = None
    else:
        ins, rest = rest[:3], rest[3:]
    dw1, dw3, dw2, xb, gb, items, sin = rest
    j = pl.program_id(0)
    w = w1.shape[1]
    ng = ns * el // ne
    for k, o in enumerate((dw1, dw3, dw2)):
        o[...] = jnp.zeros_like(o) if first else ins[k][...]

    cnt = jnp.int32(0)
    for g in range(ng):
        pos = jnp.int32(0)
        for jj in range(el):
            n = _used(meta, dims, g, jj, 0) + _used(meta, dims, g, jj, 1)
            pos = pos + jnp.where(jj < j, n, 0)
        n = _used(meta, dims, g, j, 0) + _used(meta, dims, g, j, 1)
        for q, (pre, lo, hi, c) in enumerate(parts):
            if hi is None:
                base = _total(meta, dims, g) - c
                a = jnp.maximum(pos, lo) - base
                z = pos + n - base
            else:
                a = jnp.clip(pos - lo, 0, c)
                z = jnp.clip(pos + n - lo, 0, c)

            def put(b, k, q=q, g=g, a=a, z=z, c=c):
                s = a + b * RB
                items[k, 0] = q
                items[k, 1] = g
                items[k, 2] = jnp.minimum(s, c - RB)
                items[k, 3] = s
                items[k, 4] = jnp.minimum(s + RB, z)
                return k + 1

            cnt = lax.fori_loop(0, (jnp.maximum(z - a, 0) + RB - 1) // RB, put, cnt)

    def copies(i, slot, op):
        g = items[i, 1]
        st = pl.multiple_of(items[i, 2], AL)
        for q, (pre, lo, hi, c) in enumerate(parts):
            @pl.when(items[i, 0] == q)
            def _():
                for k, dst in enumerate((xb, gb)):
                    src = arrs[2 * q + k]
                    view = src.at[g, pl.ds(st, RB)] if pre is None else src.at[g, pre[k], pl.ds(st, RB)]
                    op(pltpu.make_async_copy(view, dst.at[slot], sin.at[slot, k]))

    start = lambda cp: cp.start()
    wait = lambda cp: cp.wait()

    @pl.when(cnt > 0)
    def _():
        copies(0, 0, start)

    def step(i, carry):
        slot = lax.rem(i, 2)

        @pl.when(i + 1 < cnt)
        def _():
            copies(i + 1, 1 - slot, start)

        copies(i, slot, wait)
        row = items[i, 2] + lax.broadcasted_iota(I32, (RB, w), 0)
        keep = (row >= items[i, 3]) & (row < items[i, 4])
        x = jnp.where(keep, xb[slot].astype(F32), 0.0).astype(BF16)
        g = jnp.where(keep, gb[slot].astype(F32), 0.0).astype(BF16)
        h1f = jnp.dot(x, w1[0], preferred_element_type=F32).astype(BF16).astype(F32)
        h3f = jnp.dot(x, w3[0], preferred_element_type=F32).astype(BF16).astype(F32)
        da = _nt(g, w2[0]).astype(BF16).astype(F32)
        s = 0.5 * jnp.tanh(0.5 * h1f) + 0.5
        silu = h1f * s
        a = (silu * h3f).astype(BF16)
        dh1 = (da * h3f * (s + silu * (1.0 - s))).astype(BF16)
        dh3 = (da * silu).astype(BF16)
        dw1[0] += _tn(x, dh1)
        dw3[0] += _tn(x, dh3)
        dw2[0] += _tn(a, g)
        return carry

    lax.fori_loop(0, cnt, step, 0)


def _share(meta, arrs, parts, w1, w3, w2, prev, dims):
    ns, ne, el = dims
    ng = ns * el // ne
    w = w1.shape[1]
    fs = w1.shape[2] // ng
    di = ns * ne + 1
    cap = sum(ng * (c // RB + 2) for _, _, _, c in parts)
    in_specs = [ANY] * len(arrs) + [
        pl.BlockSpec((1, w, fs), lambda j, m: (j, 0, m[di])),
        pl.BlockSpec((1, w, fs), lambda j, m: (j, 0, m[di])),
        pl.BlockSpec((1, fs, w), lambda j, m: (j, m[di], 0))]
    acc = [pl.BlockSpec((1, w, fs), lambda j, m: (j, 0, 0)), pl.BlockSpec((1, w, fs), lambda j, m: (j, 0, 0)),
           pl.BlockSpec((1, fs, w), lambda j, m: (j, 0, 0))]
    first = prev is None
    args = (meta,) + tuple(arrs) + (w1, w3, w2) + (() if first else tuple(prev))
    na = len(arrs) + 4
    rows = ng * parts[0][3]
    return pl.pallas_call(
        functools.partial(_share_kernel, dims, parts, first),
        grid_spec=pltpu.PrefetchScalarGridSpec(
            num_scalar_prefetch=1, grid=(el,), in_specs=in_specs + ([] if first else acc), out_specs=acc,
            scratch_shapes=[pltpu.VMEM((2, RB, w), BF16), pltpu.VMEM((2, RB, w), BF16),
                            pltpu.SMEM((cap, 5), I32), pltpu.SemaphoreType.DMA((2, 2))]),
        out_shape=[jax.ShapeDtypeStruct((el, w, fs), F32), jax.ShapeDtypeStruct((el, w, fs), F32),
                   jax.ShapeDtypeStruct((el, fs, w), F32)],
        input_output_aliases={} if first else {na: 0, na + 1: 1, na + 2: 2},
        compiler_params=pltpu.CompilerParams(vmem_limit_bytes=VMEM_LIMIT),
        cost_estimate=pl.CostEstimate(flops=8 * rows * w * fs, bytes_accessed=4 * rows * w, transcendentals=0),
        name="share",
    )(*args)


def _take_kernel(tb, idx, d0, d1, o, buf, row):
    i = pl.program_id(0)
    n, w = d0.shape

    @pl.when(i == 0)
    def _():
        for k, s in enumerate((d0, d1)):
            def fill(b, c, k=k, s=s):
                buf[pl.ds(k * n + b * 64, 64), :] = s[pl.ds(b * 64, 64), :].astype(F32)
                return c

            lax.fori_loop(0, n // 64, fill, 0)
        buf[pl.ds(2 * n, 8), :] = jnp.zeros((8, w), F32)

    def step(t, c):
        for u in range(8):
            row[pl.ds(t * 8 + u, 1), :] = buf[pl.ds(idx[i * tb + t * 8 + u], 1), :]
        return c

    lax.fori_loop(0, tb // 8, step, 0)
    o[...] = row[...].astype(BF16)


def _take(idx, d0, d1, tb=512):
    n, w = d0.shape
    t = idx.shape[0]
    whole = pl.BlockSpec((n, w), lambda i, m: (0, 0), pipeline_mode=pl.Buffered(1))
    return pl.pallas_call(
        functools.partial(_take_kernel, tb),
        grid_spec=pltpu.PrefetchScalarGridSpec(
            num_scalar_prefetch=1, grid=(t // tb,), in_specs=[whole, whole],
            out_specs=pl.BlockSpec((tb, w), lambda i, m: (i, 0)),
            scratch_shapes=[pltpu.VMEM((2 * n + 8, w), F32), pltpu.VMEM((tb, w), F32)]),
        out_shape=jax.ShapeDtypeStruct((t, w), BF16),
        compiler_params=pltpu.CompilerParams(vmem_limit_bytes=48 * 1024 * 1024),
        cost_estimate=pl.CostEstimate(flops=20 * t * w, bytes_accessed=8 * n * w, transcendentals=0),
        name="take",
    )(idx, d0, d1)


def solution(mesh):
    np_ = mesh.shape['expert']
    nd = mesh.shape['data']
    tok = P(('data', 'expert'), None)
    buf = P(('data', 'expert'), None, None)
    wsp = P('expert', None, None)

    def body(dy, gates, topk_idx, slot, yd, xd, h1, h3, w1, w3, w2):
        _, d = dy.shape
        el = w1.shape[0]
        ne = np_ * el
        ns = nd * np_
        cap = xd.shape[1] // np_
        dims = (ns, ne, el)
        e = lax.axis_index('expert')
        dd = lax.axis_index('data')
        ex = topk_idx[:, 0]
        sl = slot[:, 0]
        alld = _extents(ex, sl, ne, (nd, np_))
        meta = jnp.concatenate([alld, e[None].astype(I32), dd[None].astype(I32)])
        rows = jnp.bitwise_and(alld + (AL - 1), -AL).reshape(nd, np_, np_, el).sum(axis=(1, 3))
        most = jnp.max(rows)
        pair = jnp.max(rows.sum(axis=1))
        theirs = rows[dd, 1 - e]
        rel = jnp.bitwise_xor(ex, e.astype(I32) * el)
        flat = jnp.where(sl >= 0, rel * cap + sl, ne * cap)

        swap = [(0, 1), (1, 0)]

        def gather(v):
            return lax.all_gather(v, 'data')

        def path(bounds, win, *args):
            return work(bounds, win, *args)

        def work(bounds, win, dy, gates, flat, yd, xd, h1, h3, w1, w3, w2, meta, theirs):
            half = bounds[-1]
            x2 = xd.reshape(el * np_ * cap, d)
            xl = _pack(meta, x2, x2, dims, bounds, win, True)
            xa = gather(xl[0])
            v = (gates * dy.astype(F32)).astype(BF16)
            slots, _ = lax.optimization_barrier((flat, xl[0]))
            send = jnp.zeros((ne * cap, d), BF16).at[slots].set(v, mode='drop').reshape(2, el, cap, d)
            g0 = send[0]
            g1 = lax.ppermute(send[1], 'expert', swap)
            gl = _pack(meta, g0.reshape(el * cap, d), g1.reshape(el * cap, d), dims, bounds, win, False)
            ga = gather(gl[0])
            if win:
                own_row = lax.broadcasted_iota(I32, (win, d), 0) < win - jnp.maximum(theirs - half, 0)
                top = jnp.stack([jnp.where(own_row, m[2], lax.ppermute(m[3], 'expert', swap)) for m in (xl, gl)])
                mid = jnp.stack([xl[1], gl[1]])
                ta = gather(top)
                ma = gather(mid)
                tb = lax.ppermute(ta, 'expert', swap)
            else:
                mid = jnp.stack([xl[1], gl[1]])
                ma = gather(mid)
            o0, o1 = _own(meta, g0, g1, h1, h3, w1, w3, w2, dims)
            b1 = lax.ppermute(o1, 'expert', swap)
            dx = _take(flat, o0.reshape(el * cap, d), b1.reshape(el * cap, d))
            dg = jnp.einsum('tkd,td->tk', yd, dy, preferred_element_type=F32)
            ws = (w1, w3, w2)
            acc = _share(meta, (xa, ga), [(None, 0, bounds[1], bounds[1])], *ws, None, dims)
            if win:
                acc = _share(meta, (ta, ta, tb, tb), [((0, 1), bounds[2], half, win), ((0, 1), half, None, win)], *ws, acc, dims)
            acc = _share(meta, (ma, ma), [((0, 1), bounds[1], bounds[2], bounds[2] - bounds[1])], *ws, acc, dims)
            return dx, dg, acc[0], acc[1], acc[2]

        win = 1024
        tiers = [(2816, win), (2944, win), (3136, win)]
        paths = [functools.partial(path, (0, n - w_ - 512, n - w_, n), w_) for n, w_ in tiers]
        full = np_ * cap * el
        paths.append(functools.partial(path, (0, full // 2, full), 0))
        pick = jnp.int32(0)
        for n, w_ in tiers:
            pick = pick + ((pair > 2 * n) | (most > n + w_)).astype(I32)
        return lax.switch(pick, paths, dy, gates, flat, yd, xd, h1, h3, w1, w3, w2, meta, theirs)

    return jax.shard_map(body, mesh=mesh,
                         in_specs=(tok, tok, tok, tok, buf, buf, buf, buf, wsp, wsp, wsp),
                         out_specs=(tok, tok, P('expert', None, 'data'), P('expert', None, 'data'), P('expert', 'data', None)),
                         check_vma=False)
```
